32 devices in a mesh: dp: 32 (over z, y, x, core).
Axes of the slice: x: 2, y: 2, z: 4, core: 2. Of those that a mesh axis runs over, the one named last changes fastest.
Arguments:
- img_emb: bfloat16 [32768, 512], P('dp')
- txt_emb: bfloat16 [32768, 512], P('dp')
- log_temp: float32 [], replicated
- logit_bias: float32 [], replicated
Outputs:
- output 1: float32 [], replicated
- output 2: float32 [32768, 512], P('dp')
- output 3: float32 [32768, 512], P('dp')
- output 4: float32 [], replicated
- output 5: float32 [], replicated
All inputs are finite; a program needn't handle non-finite values.
Results may differ from the reference program's by a relative error of at most 0.001.
Values are sent between devices in bfloat16 or wider.
A program may use at most 1 GiB of HBM per device.

```python
import jax
import jax.numpy as jnp
from jax import lax

EMBED_DIM = 512
ROWS_DEV = 1024
GROUP_SIZE = 32


def setup_inputs(seed: int = 0) -> dict:
    total_rows = ROWS_DEV * GROUP_SIZE
    num_groups = total_rows // 4
    unit_scale = EMBED_DIM ** -0.5
    rand_keys = jax.random.split(jax.random.key(seed), 10)
    shared_dir = jax.random.normal(rand_keys[0], (EMBED_DIM,), jnp.float32) * unit_scale
    centers = jax.random.normal(rand_keys[1], (num_groups, EMBED_DIM), jnp.float32) * unit_scale
    member = jax.random.randint(rand_keys[2], (total_rows,), 0, num_groups)
    own_part = jax.random.normal(rand_keys[3], (total_rows, EMBED_DIM), jnp.float32) * unit_scale
    img_noise = jax.random.normal(rand_keys[4], (total_rows, EMBED_DIM), jnp.float32) * unit_scale
    txt_noise = jax.random.normal(rand_keys[5], (total_rows, EMBED_DIM), jnp.float32) * unit_scale
    common = 0.47 * centers[member] + 0.28 * own_part
    img_scale = jax.random.uniform(rand_keys[6], (total_rows, 1), jnp.float32, minval=20.0, maxval=60.0)
    txt_scale = jax.random.uniform(rand_keys[7], (total_rows, 1), jnp.float32, minval=20.0, maxval=60.0)
    img_emb = (img_scale * (0.35 * shared_dir + common + 0.76 * img_noise)).astype(jnp.bfloat16)
    txt_emb = (txt_scale * (common - 0.35 * shared_dir + 0.76 * txt_noise)).astype(jnp.bfloat16)
    log_temp = jax.random.uniform(rand_keys[8], (), jnp.float32, minval=4.6, maxval=4.8)
    logit_bias = jax.random.uniform(rand_keys[9], (), jnp.float32, minval=-14.0, maxval=-10.0)
    return {"img_emb": img_emb, "txt_emb": txt_emb, "log_temp": log_temp, "logit_bias": logit_bias}


def normalize_rows(emb):
    emb32 = emb.astype(jnp.float32)
    inv_norm = lax.rsqrt(jnp.sum(emb32 * emb32, axis=-1, keepdims=True))
    return emb32 * inv_norm, inv_norm


def project_back(unit_rows, inv_norm, grad_dir):
    radial = jnp.sum(unit_rows * grad_dir, axis=-1, keepdims=True)
    return (grad_dir - unit_rows * radial) * inv_norm


def reference(img_emb, txt_emb, log_temp, logit_bias):
    total_rows = img_emb.shape[0]
    embed_width = img_emb.shape[1]
    block_rows = min(ROWS_DEV, 512)
    num_blocks = total_rows // block_rows
    img_unit, img_inv = normalize_rows(img_emb)
    txt_unit, txt_inv = normalize_rows(txt_emb)
    img_b = img_unit.astype(jnp.bfloat16)
    txt_b = txt_unit.astype(jnp.bfloat16)
    temp_scale = jnp.exp(log_temp)
    col_ids = jnp.arange(total_rows)

    def row_block(acc_state, block_in):
        x_blk, blk_idx = block_in
        loss_sum, weight_sum, weighted_sim, txt_grad = acc_state
        sim_vals = jnp.dot(x_blk, txt_b.T, preferred_element_type=jnp.float32)
        logits = temp_scale * sim_vals + logit_bias
        row_ids = blk_idx * block_rows + jnp.arange(block_rows)
        label_signs = jnp.where(row_ids[:, None] == col_ids[None, :], 1.0, -1.0)
        weights = -label_signs * jax.nn.sigmoid(-label_signs * logits)
        weights_b = weights.astype(jnp.bfloat16)
        new_state = (
            loss_sum + jnp.sum(jax.nn.softplus(-label_signs * logits)),
            weight_sum + jnp.sum(weights),
            weighted_sim + jnp.sum(weights * sim_vals),
            txt_grad + jnp.dot(weights_b.T, x_blk, preferred_element_type=jnp.float32),
        )
        return new_state, jnp.dot(weights_b, txt_b, preferred_element_type=jnp.float32)

    init_state = (
        jnp.zeros((), jnp.float32),
        jnp.zeros((), jnp.float32),
        jnp.zeros((), jnp.float32),
        jnp.zeros((total_rows, embed_width), jnp.float32),
    )
    blocks_in = (img_b.reshape(num_blocks, block_rows, embed_width), jnp.arange(num_blocks))
    final_state, img_parts = lax.scan(row_block, init_state, blocks_in)
    loss_sum, weight_sum, weighted_sim, txt_grad = final_state
    img_dir = temp_scale * img_parts.reshape(total_rows, embed_width)
    txt_dir = temp_scale * txt_grad
    loss_val = loss_sum / total_rows
    grad_img = project_back(img_unit, img_inv, img_dir)
    grad_txt = project_back(txt_unit, txt_inv, txt_dir)
    grad_log_temp = temp_scale * weighted_sim / total_rows
    grad_bias = weight_sum / total_rows
    return (loss_val, grad_img, grad_txt, grad_log_temp, grad_bias)
```

```python
import functools

import jax
import jax.numpy as jnp
from jax import lax
from jax.experimental import pallas as pl
from jax.experimental.pallas import tpu as pltpu
from jax.sharding import PartitionSpec as P

LOG2E = 1.4426950408889634
LN2 = 0.6931471805599453
NT_DIMS = (((1,), (1,)), ((), ()))
TN_DIMS = (((0,), (0,)), ((), ()))
ROWS = 1024
HALF = 512
WIDTH = 512

PARTS = 2
TASKS = (0, 8, 4, 12, 36, 32, 37, 9, 13, 24, 48, 53, 52, 33, 50, 49, 38, 29, 54, 21, 19, 51, 3, 23, 55, 31, 11, 43, 39, 61, 40, 59, 60, 57, 15, 7, 34, 63, 56, 58, 62, 47, 27, 35, 28, 44, 46, 1, 41, 42, 25, 45, 14, 26, 5, 30, 6, 10, 22, 17, 18, 2, 20, 16)
EVENTS = (
    (3, 'ty', 0),
    (3, 'iz', 0),
    (3, 'tz', 0),
    (3, 'ty', 1),
    (9, 'tyz', 0),
    (13, 'iz', 1),
    (13, 'tz', 1),
    (19, 'tyz', 1),
    (25, 'ux', 3, 0, 0),
    (25, 'ux', 3, 0, 1),
    (41, 'ux', 3, 1, 0),
    (41, 'ux', 3, 1, 1),
    (42, 'vc', 3),
    (44, 'uz', 0, 0),
    (44, 'uz', 0, 1),
    (44, 'vy', 3, 0, 0),
    (44, 'vy', 3, 0, 1),
    (44, 'vy', 3, 1, 0),
    (44, 'vy', 3, 1, 1),
    (52, 'uz', 1, 0),
    (52, 'uz', 1, 1),
    (55, 'vc', 1),
    (56, 'ux', 1, 1, 0),
    (56, 'ux', 1, 1, 1),
    (59, 'vc', 2),
    (60, 'vy', 1, 0, 0),
    (60, 'vy', 1, 0, 1),
    (60, 'vy', 1, 1, 0),
    (60, 'vy', 1, 1, 1),
    (62, 'vz', 0, 0),
    (62, 'vz', 0, 1),
    (62, 'vz', 1, 0),
    (62, 'vz', 1, 1),
    (63, 'vc', 0),
    (64, 'ux', 1, 0, 0),
    (64, 'ux', 1, 0, 1),
)
PIECE = HALF // PARTS
COPIES = {}


def _register():
    names = []
    for h in range(2):
        names += [("ix", h), ("iz", h), ("ixz", h), ("ty", h), ("tz", h), ("tyz", h)]
        names += [("tc", q, h) for q in range(4)]
        for p in range(PARTS):
            names += [("ux", 1, h, p), ("ux", 3, h, p), ("uz", h, p)]
            names += [("vy", 1, h, p), ("vy", 3, h, p), ("vz", h, p)]
    names += [("vc", q) for q in range(4)]
    names += [("st", k) for k in range(5)]
    for k, n in enumerate(names):
        COPIES[n] = k


_register()


def flip(me, bit):
    return me + bit - 2 * bit * lax.rem(lax.div(me, bit), 2)


def task_at(t):
    per = 5
    words = []
    for k in range(0, len(TASKS), per):
        word = 0
        for pos, code in enumerate(TASKS[k:k + per]):
            word |= code << (6 * pos)
        words.append(word)
    which, pos = lax.div(t, per), lax.rem(t, per)
    word = jnp.int32(words[0])
    for k in range(1, len(words)):
        word = jnp.where(which == k, jnp.int32(words[k]), word)
    code = jnp.int32(0)
    for k in range(per):
        code = jnp.where(pos == k, lax.rem(lax.div(word, jnp.int32(64 ** k)), 64), code)
    return lax.div(code, 8), lax.rem(code, 8)


def pair_kernel(sc_ref, xin, yin, u_out, v_out, st_out,
                X, Y, U, V, RX, RZ, RC, RY, RZ2, S, sums, ST, RS, send, recv, local):
    me = lax.axis_index("dp")
    core, xn, yn, z1, z2 = peers = [flip(me, b) for b in (1, 2, 4, 8, 16)]
    ts2, b2 = sc_ref[0], sc_ref[1]

    barrier = pltpu.get_barrier_semaphore()
    loads = [pltpu.make_async_copy(xin, X.at[pl.ds(0, ROWS)], local.at[0]),
             pltpu.make_async_copy(yin, Y.at[pl.ds(0, ROWS)], local.at[1])]
    for load in loads:
        load.start()
    for peer in peers:
        pl.semaphore_signal(barrier, inc=1, device_id=(peer,), device_id_type=pl.DeviceIdType.MESH)
    pl.semaphore_wait(barrier, 5)
    for load in loads:
        load.wait()

    def rows(block, h):
        return pl.ds(block * ROWS + h * HALF, HALF)

    def part(block, h, p):
        return pl.ds(block * ROWS + h * HALF + p * PIECE, PIECE)

    def copy(*name):
        kind, tail = name[0], name[1:]
        if kind == "ix":
            src, dst, dev = X.at[rows(0, *tail)], X.at[rows(1, *tail)], xn
        elif kind == "iz":
            src, dst, dev = X.at[rows(0, *tail)], X.at[rows(2, *tail)], z2
        elif kind == "ixz":
            src, dst, dev = X.at[rows(2, *tail)], X.at[rows(3, *tail)], xn
        elif kind == "ty":
            src, dst, dev = Y.at[rows(0, *tail)], Y.at[rows(1, *tail)], yn
        elif kind == "tz":
            src, dst, dev = Y.at[rows(0, *tail)], Y.at[rows(2, *tail)], z1
        elif kind == "tyz":
            src, dst, dev = Y.at[rows(2, *tail)], Y.at[rows(3, *tail)], yn
        elif kind == "tc":
            src, dst, dev = Y.at[rows(*tail)], Y.at[rows(4 + tail[0], tail[1])], core
        elif kind == "ux":
            src, dst, dev = U.at[part(*tail)], RX.at[part(tail[0] // 2, *tail[1:])], xn
        elif kind == "uz":
            src, dst, dev = U.at[part(2, *tail)], RZ.at[part(0, *tail)], z2
        elif kind == "vc":
            src = V.at[pl.ds((4 + tail[0]) * ROWS, ROWS)]
            dst, dev = RC.at[pl.ds(tail[0] * ROWS, ROWS)], core
        elif kind == "vy":
            src, dst, dev = V.at[part(*tail)], RY.at[part(tail[0] // 2, *tail[1:])], yn
        elif kind == "vz":
            src, dst, dev = V.at[part(2, *tail)], RZ2.at[part(0, *tail)], z1
        else:
            src, dst, dev = ST.at[tail[0]], RS.at[tail[0]], peers[tail[0]]
        k = COPIES[name]
        return pltpu.make_async_remote_copy(src_ref=src, dst_ref=dst, send_sem=send.at[k], recv_sem=recv.at[k],
                                            device_id=(dev,), device_id_type=pl.DeviceIdType.MESH)

    start = lambda *name: copy(*name).start()
    arrived = lambda *name: copy(*name).wait_recv()

    for h in range(2):
        start("tc", 0, h)
    for h in range(2):
        start("ix", h)
        start("ty", h)
        start("iz", h)
        start("tz", h)

    def clear(k, carry):
        r = pl.ds(pl.multiple_of(k * 256, 256), 256)
        U[r, :] = jnp.zeros((256, WIDTH), jnp.float32)
        V[r, :] = jnp.zeros((256, WIDTH), jnp.float32)
        V[pl.ds(pl.multiple_of(4096 + k * 256, 256), 256), :] = jnp.zeros((256, WIDTH), jnp.float32)
        return carry

    lax.fori_loop(0, 16, clear, 0)
    sums[...] = jnp.zeros_like(sums)

    def spans(t):
        i, j = task_at(t)
        return pl.ds(pl.multiple_of(i * HALF, HALF), HALF), pl.ds(pl.multiple_of(j * ROWS, ROWS), ROWS)

    def logits(t):
        ri, rj = spans(t)
        return lax.dot_general(X[ri, :], Y[rj, :], NT_DIMS, preferred_element_type=jnp.float32)

    def weigh(diag_offset):
        s = S[...]
        m = s * ts2 + b2
        if diag_offset is not None:
            row = lax.broadcasted_iota(jnp.int32, s.shape, 0) + diag_offset
            on_diag = row == lax.broadcasted_iota(jnp.int32, s.shape, 1)
            m = jnp.where(on_diag, -m, m)
        e = jnp.exp2(-jnp.abs(m))
        q = 1.0 + e
        h = jnp.where(m >= 0, 1.0, e) * (1.0 / q)
        if diag_offset is not None:
            h = jnp.where(on_diag, -h, h)
        groups = lambda a: a.reshape(HALF // 8, 8, ROWS)
        sums[0] += jnp.sum(groups(h), axis=0)
        sums[1] += jnp.sum(groups(h * s), axis=0)
        sums[2] += jnp.sum(groups(jnp.maximum(m, 0.0)), axis=0)
        e3, q3 = groups(e), groups(q)
        p = e3[0]
        for k in range(1, HALF // 8):
            p = p * q3[k] + e3[k]
        sums[3] += jnp.log1p(p)
        return h.astype(jnp.bfloat16)

    def step(t, diag_offset=None):
        ri, rj = spans(t)
        hb = weigh(diag_offset)
        S[...] = logits(jnp.minimum(t + 1, len(TASKS) - 1))
        U[ri, :] += jnp.dot(hb, Y[rj, :], preferred_element_type=jnp.float32)
        V[rj, :] += lax.dot_general(hb, X[ri, :], TN_DIMS, preferred_element_type=jnp.float32)

    def add_into(dst, d0, src, s0, n):
        def body(k, carry):
            d = pl.ds(pl.multiple_of(d0 + k * 128, 128), 128)
            dst[d, :] += src[pl.ds(pl.multiple_of(s0 + k * 128, 128), 128), :]
            return carry
        lax.fori_loop(0, n // 128, body, 0)

    def at(block, h, p):
        return block * ROWS + h * HALF + p * PIECE

    first = {}
    for k, code in enumerate(TASKS):
        first.setdefault(("I", code // 8), k)
        first.setdefault(("T", code % 8), k)

    relays = {("ty", h): [("tc", 1, h)] for h in range(2)}
    relays.update({("tz", h): [("tyz", h), ("tc", 2, h)] for h in range(2)})
    relays.update({("tyz", h): [("tc", 3, h)] for h in range(2)})
    relays.update({("iz", h): [("ixz", h)] for h in range(2)})

    def perform(*name):
        kind, tail = name[0], name[1:]
        if name in relays:
            arrived(*name)
            for out in relays[name]:
                start(*out)
            return
        if kind == "uz":
            h, p = tail
            arrived("ux", 3, h, p)
            add_into(U, at(2, h, p), RX, at(1, h, p), PIECE)
        elif kind == "vy":
            q, h, p = tail
            if (h, p) == (0, 0):
                arrived("vc", q)
            add_into(V, at(q, h, p), RC, at(q, h, p), PIECE)
        elif kind == "vz":
            h, p = tail
            if (h, p) == (0, 0):
                arrived("vc", 2)
            arrived("vy", 3, h, p)
            add_into(V, at(2, h, p), RC, at(2, h, p), PIECE)
            add_into(V, at(2, h, p), RY, at(1, h, p), PIECE)
        start(*name)

    before = {}
    act = lambda k, fn: before.setdefault(k, []).append(fn)
    for k, *name in EVENTS:
        act(k, functools.partial(perform, *name))
    inputs = {("I", 2): [("ix", 0)], ("I", 3): [("ix", 1)], ("I", 6): [("ixz", 0)], ("I", 7): [("ixz", 1)]}
    inputs.update({("T", 4 + q): [("tc", q, 0), ("tc", q, 1)] for q in range(4)})
    for key, names in inputs.items():
        for name in names:
            act(max(first[key] - 1, 0), functools.partial(arrived, *name))

    def run_actions(k):
        for fn in before.get(k, []):
            fn()

    S[...] = logits(jnp.int32(0))

    def diag_body(t, carry):
        for k in (0, 1):
            if k in before:
                pl.when(t == k)(functools.partial(run_actions, k))
        step(t, t * HALF)
        return carry

    lax.fori_loop(0, 2, diag_body, 0)

    def body(t, carry):
        for k in sorted(before):
            if 2 <= k < 64:
                pl.when(t == k)(functools.partial(run_actions, k))
        step(t)
        return carry

    lax.fori_loop(2, 64, body, 0)
    run_actions(64)

    outs = []
    pieces = [(h, p) for h in range(2) for p in range(PARTS)]
    for h, p in pieces:
        arrived("ux", 1, h, p)
        add_into(U, at(0, h, p), RX, at(0, h, p), PIECE)
    arrived("vc", 0)
    for h, p in pieces:
        arrived("vy", 1, h, p)
        add_into(V, at(0, h, p), RC, at(0, h, p), PIECE)
        add_into(V, at(0, h, p), RY, at(0, h, p), PIECE)
    for h, p in pieces:
        for kind, dst, src, out in (("uz", U, RZ, u_out), ("vz", V, RZ2, v_out)):
            arrived(kind, h, p)
            add_into(dst, at(0, h, p), src, at(0, h, p), PIECE)
            r = part(0, h, p)
            outs.append(pltpu.make_async_copy(dst.at[r], out.at[r], local.at[2 + len(outs)]))
            outs[-1].start()

    kind_row = lax.broadcasted_iota(jnp.int32, (8, 128), 0)
    mine = jnp.zeros((8, 128), jnp.float32)
    for k in range(4):
        total = sums[k, :, 0:128]
        for c in range(128, ROWS, 128):
            total = total + sums[k, :, c:c + 128]
        mine = jnp.where(kind_row == k, jnp.sum(total, axis=0, keepdims=True), mine)
    for k in range(5):
        ST[k] = mine
        start("st", k)
        arrived("st", k)
        mine = mine + RS[k]
    st_out[...] = mine
    for out in outs:
        out.wait()
    for name in COPIES:
        copy(*name).wait_send()


def normalize_rows(emb):
    emb32 = emb.astype(jnp.float32)
    inv_norm = lax.rsqrt(jnp.sum(emb32 * emb32, axis=-1, keepdims=True))
    return emb32 * inv_norm, inv_norm


def project_back(unit_rows, inv_norm, grad_dir):
    radial = jnp.sum(unit_rows * grad_dir, axis=-1, keepdims=True)
    return (grad_dir - unit_rows * radial) * inv_norm


def solution(mesh):
    total_rows = ROWS * mesh.shape["dp"]
    f32 = lambda *shape: jax.ShapeDtypeStruct(shape, jnp.float32)
    acc = lambda n, dtype=jnp.float32: pltpu.VMEM((n, WIDTH), dtype)
    hbm = pl.BlockSpec(memory_space=pl.ANY)
    n_copies = len(COPIES)

    def local_fn(img_emb, txt_emb, log_temp, logit_bias):
        img_unit, img_inv = normalize_rows(img_emb)
        txt_unit, txt_inv = normalize_rows(txt_emb)
        temp_scale = jnp.exp(log_temp)
        scalars = jnp.stack([temp_scale * LOG2E, logit_bias * LOG2E])
        u_sum, v_sum, st = pl.pallas_call(
            pair_kernel,
            out_shape=[f32(ROWS, WIDTH), f32(ROWS, WIDTH), f32(8, 128)],
            in_specs=[pl.BlockSpec(memory_space=pltpu.SMEM), hbm, hbm],
            out_specs=[hbm, hbm, pl.BlockSpec(memory_space=pltpu.VMEM)],
            scratch_shapes=[
                acc(4096, jnp.bfloat16), acc(8192, jnp.bfloat16), acc(4096), acc(8192),
                acc(2048), acc(1024), acc(4096), acc(2048), acc(1024),
                pltpu.VMEM((HALF, ROWS), jnp.float32), pltpu.VMEM((4, 8, ROWS), jnp.float32),
                pltpu.VMEM((5, 8, 128), jnp.float32), pltpu.VMEM((5, 8, 128), jnp.float32),
                pltpu.SemaphoreType.DMA((n_copies,)), pltpu.SemaphoreType.DMA((n_copies,)),
                pltpu.SemaphoreType.DMA((2 + 4 * PARTS,)),
            ],
            compiler_params=pltpu.CompilerParams(collective_id=0, has_side_effects=True, vmem_limit_bytes=67043328),
        )(scalars, img_unit.astype(jnp.bfloat16), txt_unit.astype(jnp.bfloat16))
        sums = jnp.sum(st, axis=1) / total_rows
        loss = sums[3] + LN2 * sums[2]
        grad_img = project_back(img_unit, img_inv, temp_scale * u_sum)
        grad_txt = project_back(txt_unit, txt_inv, temp_scale * v_sum)
        return loss, grad_img, grad_txt, temp_scale * sums[1], sums[0]

    return jax.shard_map(
        local_fn,
        mesh=mesh,
        in_specs=(P("dp", None), P("dp", None), P(), P()),
        out_specs=(P(), P("dp", None), P("dp", None), P(), P()),
        check_vma=False,
    )
```
